256 devices in a mesh: cuts: 8 (over z_hi, x), row: 32 (over z_lo, y, core).
Axes of the slice: x: 4, y: 4, z: 8 (z_hi: 2, z_lo: 4; z = z_hi * 4 + z_lo), core: 2. Of those that a mesh axis runs over, the one named last changes fastest.
Arguments:
- raw: bfloat16 [8, 3, 5, 1024, 1024], P('cuts', None, None, 'row'), may hold values from -6 to 6
- otf: float32 [8, 1024, 1024], P('cuts', 'row'), may hold values from 0.0135 to 121.5, as said below
- offsets: int32 [3, 2], replicated, may hold values from -256 to 255
- phase_order: int32 [3, 5], replicated, may hold values from 0 to 4, each once within a row
- unmix: float32 [2, 3, 5, 5], replicated, may hold values from -3 to 3
Outputs:
- recon: float32 [8, 1024, 1024], P('cuts', 'row')
The draws below stay inside these ranges and needn't reach their ends.
Inputs may be any that keep to these rules, and one draw needn't show every extreme that they name: `otf`: positive.
All inputs are finite; a program needn't handle non-finite values.
Results may differ from the reference program's by a relative error of at most 0.0072.
Values may be sent and summed in bfloat16 or wider, within the bound.
A program may use at most 128 MiB of HBM per device.

```python
import math
import jax
import jax.numpy as jnp
from jax import lax

N = 1024
ANGLES = 3
PHASES = 5
BANDS = 5
SLICES = 8


def draw_otf(key, part):
    first = jax.random.fold_in(jax.random.fold_in(key, 11), 0)
    depth = jnp.arange(SLICES, dtype=jnp.float32) / max(SLICES - 1, 1)
    base = jnp.exp(jax.random.uniform(first, (SLICES, N, N), jnp.float32, math.log(0.15), math.log(1.5)))
    ramp = jnp.exp(depth * math.log(3.0))
    return base * ramp[:, None, None]


def with_ends(entries, key, least, largest):
    longest = entries.shape.index(max(entries.shape))
    spots = []
    for shift in (0, 1):
        where = [jax.random.randint(jax.random.fold_in(key, axis), (), 0, length) for axis, length in enumerate(entries.shape)]
        where[longest] = (where[longest] + shift) % entries.shape[longest]
        spots.append(tuple(where))
    return entries.at[spots[0]].set(least).at[spots[1]].set(largest)


def shard_levels(key, dims, pieces, smallest, high):
    def one(dim, blocks):
        heights = jax.random.uniform(jax.random.fold_in(jax.random.fold_in(key, 6), dim), (blocks,), jnp.float32, smallest / len(pieces), high / len(pieces))
        return jnp.repeat(jnp.exp(heights), dims[dim] // blocks).reshape((-1,) + (1,) * (len(dims) - dim - 1))

    gain = one(*pieces[0])
    for cut in pieces[1:]:
        gain = gain * one(*cut)
    return gain


def bell_draw(stream_key, dims, spread, limit, shards=(), held_as=jnp.bfloat16):
    array = jax.random.normal(stream_key, dims, jnp.float32) * spread
    if len(shards) > 0:
        array = shard_levels(stream_key, dims, shards, -0.22, 0.18) * array
    return jnp.clip(array, min=-limit, max=limit).astype(held_as)


def setup_inputs(seed: int = 0) -> dict:
    arg_keys = jax.random.split(jax.random.key(seed), 6)
    return {
        "raw": bell_draw(arg_keys[0], (SLICES, ANGLES, PHASES, N, N), 1.0, 6.0, ((0, 8), (3, 32))),
        "otf": draw_otf(jax.random.fold_in(arg_keys[5], 71), 0),
        "offsets": with_ends(jax.random.randint(arg_keys[2], (ANGLES, 2), 0 - N // 4, N // 4), jax.random.fold_in(arg_keys[2], 1), 0 - N // 4, (N // 4) - 1).astype(jnp.int32),
        "phase_order": jax.vmap(lambda own: jax.random.permutation(own, PHASES))(jax.random.split(arg_keys[3], ANGLES)).reshape((ANGLES, PHASES)).astype(jnp.int32),
        "unmix": bell_draw(arg_keys[4], (2, ANGLES, BANDS, PHASES), 0.45, 3.0, (), jnp.float32),
    }


MULTIPLES = (0, 1, -1, 2, -2)
WIENER = 0.1

def tables(pixels):
    indices = jnp.arange(pixels, dtype=jnp.int32)
    product = indices[:, None] * indices[None, :] % pixels
    phase = product.astype(jnp.float32) * (2.0 * math.pi / pixels)
    factor = 1.0 / math.sqrt(pixels)
    return ((jnp.cos(phase) * factor).astype(jnp.bfloat16), (jnp.sin(phase) * factor).astype(jnp.bfloat16))

def mixing(unmix, phase_order):
    phases = unmix.shape[-1]
    onehot = (phase_order[:, :, None] == jnp.arange(phases, dtype=jnp.int32)[None, None, :]).astype(jnp.float32)
    highest = lax.Precision.HIGHEST
    mix_re = jnp.einsum('amp,ajp->amj', unmix[0], onehot, precision=highest)
    mix_im = jnp.einsum('amp,ajp->amj', unmix[1], onehot, precision=highest)
    return (mix_re, mix_im)

def reference(raw, otf, offsets, phase_order, unmix):
    highest = lax.Precision.HIGHEST
    cosine, sine = tables(N)
    cos_wide = cosine.astype(jnp.float32)
    sin_wide = sine.astype(jnp.float32)
    mix_re, mix_im = mixing(unmix, phase_order)
    squares = lax.optimization_barrier(jnp.sum(otf * otf, axis=0))
    power = jnp.zeros((N, N), jnp.float32)
    for which_angle in range(ANGLES):
        for band_index in range(BANDS):
            power = power + jnp.roll(squares, (MULTIPLES[band_index] * offsets[which_angle, 0], MULTIPLES[band_index] * offsets[which_angle, 1]), axis=(0, 1))
    denom = WIENER + power / (SLICES * ANGLES)

    def one_slice(pair):
        frames, response_base = pair
        frames_wide = frames.astype(jnp.float32)
        spec_re = jnp.einsum('apyx,xk->apyk', frames_wide, cos_wide, precision=highest)
        spec_im = -jnp.einsum('apyx,xk->apyk', frames_wide, sin_wide, precision=highest)
        band_re = jnp.einsum('amj,ajyk->amyk', mix_re, spec_re, precision=highest) - jnp.einsum('amj,ajyk->amyk', mix_im, spec_im, precision=highest)
        band_im = jnp.einsum('amj,ajyk->amyk', mix_re, spec_im, precision=highest) + jnp.einsum('amj,ajyk->amyk', mix_im, spec_re, precision=highest)
        numer_re = jnp.zeros((N, N), jnp.float32)
        numer_im = jnp.zeros((N, N), jnp.float32)
        for which_angle in range(ANGLES):
            for band_index in range(BANDS):
                row_shift = MULTIPLES[band_index] * offsets[which_angle, 0]
                col_shift = MULTIPLES[band_index] * offsets[which_angle, 1]
                part_re = jnp.roll(band_re[which_angle, band_index], col_shift, axis=1).astype(jnp.bfloat16).astype(jnp.float32)
                part_im = jnp.roll(band_im[which_angle, band_index], col_shift, axis=1).astype(jnp.bfloat16).astype(jnp.float32)
                col_re = jnp.dot(cos_wide, part_re, precision=highest) + jnp.dot(sin_wide, part_im, precision=highest)
                col_im = jnp.dot(cos_wide, part_im, precision=highest) - jnp.dot(sin_wide, part_re, precision=highest)
                col_re = jnp.roll(col_re, row_shift, axis=0)
                col_im = jnp.roll(col_im, row_shift, axis=0)
                response = jnp.roll(response_base, (row_shift, col_shift), axis=(0, 1))
                numer_re = numer_re + response * col_re
                numer_im = numer_im + response * col_im
        ratio_re = (numer_re / denom).astype(jnp.bfloat16).astype(jnp.float32)
        ratio_im = (numer_im / denom).astype(jnp.bfloat16).astype(jnp.float32)
        half_re = (jnp.dot(cos_wide, ratio_re, precision=highest) - jnp.dot(sin_wide, ratio_im, precision=highest)).astype(jnp.bfloat16).astype(jnp.float32)
        half_im = (jnp.dot(cos_wide, ratio_im, precision=highest) + jnp.dot(sin_wide, ratio_re, precision=highest)).astype(jnp.bfloat16).astype(jnp.float32)
        return jnp.dot(half_re, cos_wide, precision=highest) - jnp.dot(half_im, sin_wide, precision=highest)
    return lax.map(one_slice, (raw, otf))
```

```python
import math

import jax
import jax.numpy as jnp
import numpy as np
from jax import lax
from jax.experimental import pallas as pl
from jax.experimental.pallas import tpu as pltpu
from jax.sharding import PartitionSpec as P

MESH = pl.DeviceIdType.MESH
WIENER = 0.1
N = 1024
LANES = 128
TILES = N // LANES
ANGLES = 3
PHASES = 5
BANDS = 5
FIELDS = 1 + ANGLES * (BANDS - 1)
PLANES = 2 * FIELDS
SLAB = 32
ROW = 32
GROUP = 8
DEPTH = 4
CUTS = 8
PAD = 128
MULTIPLES = (0, 1, -1, 2, -2)
F32 = jnp.float32
BF16 = jnp.bfloat16


def table():
    index = np.arange(N, dtype=np.int64)
    product = (index[:, None] * index[None, :]) % N
    phase = product.astype(np.float32) * np.float32(2.0 * math.pi / N)
    factor = np.float32(1.0 / math.sqrt(N))
    both = np.concatenate([np.cos(phase) * factor, np.sin(phase) * factor], axis=1)
    return both.astype(jnp.bfloat16).reshape(GROUP, DEPTH, 2, 16, 2 * N)


def field_of(angle, band):
    return 0 if band == 0 else 1 + 4 * angle + band - 1


def lane_index(rows):
    return lax.broadcasted_iota(jnp.int32, (rows, LANES), 1)


def rows_kernel(offsets, order, unmix, raw, tab, otf, bands, otf_out, spec, band):
    for n in range(8):
        cols = pl.ds(n * 256, 256)
        rhs = tab[:, :, :, :, cols].reshape(N, 256)
        spec[:, cols] = jnp.dot(raw[...], rhs, preferred_element_type=F32)

    def mix_tile(n, carry):
        at_c = pl.ds(pl.multiple_of(n * LANES, LANES), LANES)
        at_s = pl.ds(pl.multiple_of(n * LANES + N, LANES), LANES)
        for half in range(2):
            low = [None, None]
            rows = pl.ds(half * 16, 16)
            for a in range(ANGLES):
                c, s = [], []
                for j in range(PHASES):
                    frame = pl.ds((a * PHASES + j) * SLAB + half * 16, 16)
                    c.append(spec[frame, at_c])
                    s.append(spec[frame, at_s])
                for m in range(BANDS):
                    re = im = None
                    for j in range(PHASES):
                        where = (a * BANDS + m) * PHASES + order[a * PHASES + j]
                        wr = unmix[where]
                        wi = unmix[where + ANGLES * BANDS * PHASES]
                        pr = wr * c[j] + wi * s[j]
                        pi = wi * c[j] - wr * s[j]
                        re = pr if re is None else re + pr
                        im = pi if im is None else im + pi
                    if m == 0:
                        low[0] = re if low[0] is None else low[0] + re
                        low[1] = im if low[1] is None else low[1] + im
                    else:
                        f = field_of(a, m)
                        band[2 * f, n, rows, :] = re
                        band[2 * f + 1, n, rows, :] = im
            bands[n, 0, rows, :] = low[0].astype(BF16)
            bands[n, 1, rows, :] = low[1].astype(BF16)
        return carry

    lax.fori_loop(0, TILES, mix_tile, 0)
    lane = lane_index(SLAB)
    for a in range(ANGLES):
        for m in range(1, BANDS):
            f = field_of(a, m)
            shift = lax.rem(MULTIPLES[m] * offsets[2 * a + 1] + 2 * N, N)
            whole = lax.div(shift, LANES)
            rest = lax.rem(shift, LANES)
            early = lane < LANES - rest
            for b in range(TILES):
                first = lax.rem(b - whole + TILES, TILES)
                second = lax.rem(b - whole - 1 + 2 * TILES, TILES)
                for p in (2 * f, 2 * f + 1):
                    piece = jnp.where(early, band[p, first], band[p, second])
                    bands[b, p] = pltpu.roll(piece, rest, 1).astype(BF16)
    for b in range(TILES):
        otf_out[b] = otf[:, b * LANES : (b + 1) * LANES].astype(BF16)


def rows_call(offsets, order, unmix, raw, tab, otf):
    smem = pl.BlockSpec(memory_space=pltpu.SMEM)
    vmem = pl.BlockSpec(memory_space=pltpu.VMEM)
    return pl.pallas_call(
        rows_kernel,
        name="row_spectra",
        out_shape=(
            jax.ShapeDtypeStruct((GROUP, PLANES, SLAB, LANES), BF16),
            jax.ShapeDtypeStruct((TILES, SLAB, LANES), BF16),
        ),
        in_specs=[smem, smem, smem, vmem, vmem, vmem],
        out_specs=(vmem, vmem),
        scratch_shapes=[
            pltpu.VMEM((ANGLES * PHASES * SLAB, 2 * N), F32),
            pltpu.VMEM((PLANES, TILES, SLAB, LANES), F32),
        ],
    )(offsets, order, unmix, raw, tab, otf)


def exchange_kernel(
    bands, otf, bands_out, otf_out,
    band_send, band_recv, own_sem, y_send, y_recv, z_send, z_recv, d_send, d_recv,
):
    r = lax.axis_index("row")
    z, i = r // GROUP, r % GROUP
    y, c = i // 2, i % 2
    partner = r + 1 - 2 * c

    barrier = pltpu.get_barrier_semaphore()
    for o in range(1, GROUP):
        peer = z * GROUP + lax.rem(i + o, GROUP)
        pl.semaphore_signal(barrier, inc=1, device_id={"row": peer}, device_id_type=MESH)
    for o in range(1, DEPTH):
        peer = lax.rem(z + o, DEPTH) * GROUP + i
        pl.semaphore_signal(barrier, inc=1, device_id={"row": peer}, device_id_type=MESH)
    pl.semaphore_wait(barrier, GROUP - 1 + DEPTH - 1)

    def remote(src, dst, send, recv, peer):
        copy = pltpu.make_async_remote_copy(
            src_ref=src, dst_ref=dst, send_sem=send, recv_sem=recv,
            device_id={"row": peer}, device_id_type=MESH,
        )
        copy.start()
        return copy

    own_otf = pltpu.make_async_copy(otf, otf_out.at[z, y, c], own_sem.at[0])
    own_otf.start()
    y_copies = []
    for o in range(1, DEPTH):
        peer = z * GROUP + lax.rem(y + o, DEPTH) * 2 + c
        y_copies.append(remote(otf, otf_out.at[z, y, c], y_send.at[o], y_recv.at[o], peer))
    own_bands = pltpu.make_async_copy(bands.at[i], bands_out.at[i], own_sem.at[1])
    own_bands.start()
    band_copies = []
    for o in range(1, GROUP):
        to = lax.rem(i + o, GROUP)
        band_copies.append(
            remote(bands.at[to], bands_out.at[i], band_send.at[o], band_recv.at[o], z * GROUP + to)
        )
    own_otf.wait()
    for copy in y_copies:
        copy.wait()
    z_copies = []
    for o in range(1, DEPTH):
        peer = lax.rem(z + o, DEPTH) * GROUP + i
        part = otf_out.at[z, :, c]
        z_copies.append(remote(part, part, z_send.at[o], z_recv.at[o], peer))
    d_copies = []
    part = otf_out.at[z, :, c]
    d_copies.append(remote(part, part, d_send.at[0], d_recv.at[0], partner))
    for o in range(1, DEPTH):
        z_copies[o - 1].wait_recv()
        source = lax.rem(z - o + DEPTH, DEPTH)
        part = otf_out.at[source, :, c]
        d_copies.append(remote(part, part, d_send.at[o], d_recv.at[o], partner))
    for copy in z_copies:
        copy.wait_send()
    for copy in d_copies:
        copy.wait()
    own_bands.wait()
    for copy in band_copies:
        copy.wait()


def exchange_call(bands, otf):
    vmem = pl.BlockSpec(memory_space=pltpu.VMEM)
    anywhere = pl.BlockSpec(memory_space=pl.ANY)
    dma = pltpu.SemaphoreType.DMA
    return pl.pallas_call(
        exchange_kernel,
        name="band_exchange",
        out_shape=(
            jax.ShapeDtypeStruct((GROUP, PLANES, SLAB, LANES), BF16),
            jax.ShapeDtypeStruct((DEPTH, DEPTH, 2, TILES, SLAB, LANES), BF16),
        ),
        in_specs=[vmem, vmem],
        out_specs=(anywhere, anywhere),
        scratch_shapes=[
            dma((GROUP,)), dma((GROUP,)), dma((2,)),
            dma((DEPTH,)), dma((DEPTH,)), dma((DEPTH,)), dma((DEPTH,)), dma((DEPTH,)), dma((DEPTH,)),
        ],
        compiler_params=pltpu.CompilerParams(collective_id=0, has_side_effects=True),
    )(bands, otf)


def columns_kernel(place, offsets, bands, otf, tab_c, tab_s, numer, power, resp, prod, flip):
    z, i = place[0], place[1]
    lane = lane_index(N)

    def window(f, shift):
        start = lax.rem(i * LANES - shift + 2 * N, N)
        first = lax.div(start, LANES)
        rest = lax.rem(start, LANES)
        second = lax.rem(first + 1, TILES)
        back = lax.rem(LANES - rest, LANES)
        near = otf[:, first].reshape(N, LANES).astype(F32)
        far = otf[:, second].reshape(N, LANES).astype(F32)
        piece = pltpu.roll(jnp.where(lane >= rest, near, far), back, 1)
        resp[f, 0:N, :] = piece
        resp[f, N : N + PAD, :] = piece[0:PAD]

    window(0, 0)
    for a in range(ANGLES):
        for m in range(1, BANDS):
            window(field_of(a, m), MULTIPLES[m] * offsets[2 * a + 1])

    lhs_c = tab_c[...].reshape(N, 2 * LANES)
    lhs_s = tab_s[...].reshape(N, 2 * LANES)

    def transform(f, carry):
        re = bands[:, 2 * f].reshape(GROUP * SLAB, LANES)
        im = bands[:, 2 * f + 1].reshape(GROUP * SLAB, LANES)
        upper = jnp.concatenate([re, im], axis=1)
        lower = jnp.concatenate([im, -re], axis=1)
        for part in range(4):
            rows = slice(part * 256, (part + 1) * 256)
            both = jnp.dot(lhs_c[rows], upper, preferred_element_type=F32) + jnp.dot(
                lhs_s[rows], lower, preferred_element_type=F32
            )
            weight = resp[f, part * 256 : (part + 1) * 256, :]
            out_re = both[:, :LANES] * weight
            out_im = both[:, LANES:] * weight
            prod[2 * f, part * 256 : (part + 1) * 256, :] = out_re
            prod[2 * f + 1, part * 256 : (part + 1) * 256, :] = out_im
            if part == 0:
                prod[2 * f, N : N + PAD, :] = out_re[0:PAD]
                prod[2 * f + 1, N : N + PAD, :] = out_im[0:PAD]
        return carry

    lax.fori_loop(0, FIELDS, transform, 0)

    def gather(n, carry):
        base = n * LANES
        at = pl.ds(pl.multiple_of(base, LANES), LANES)
        re = prod[0, at, :]
        im = prod[1, at, :]
        own = resp[0, at, :]
        pw = own * own * float(ANGLES)
        for a in range(ANGLES):
            for m in range(1, BANDS):
                f = field_of(a, m)
                start = lax.rem(base - MULTIPLES[m] * offsets[2 * a] + 2 * N, N)
                shifted = pl.ds(start, LANES)
                re = re + prod[2 * f, shifted, :]
                im = im + prod[2 * f + 1, shifted, :]
                own = resp[f, shifted, :]
                pw = pw + own * own
        numer[:, 0, :, at] = re.T.astype(BF16).reshape(DEPTH, SLAB, LANES)
        numer[:, 1, :, at] = im.T.astype(BF16).reshape(DEPTH, SLAB, LANES)
        flip[...] = pw.T
        power[n] = flip[pl.ds(pl.multiple_of(z * SLAB, SLAB), SLAB), :]
        return carry

    lax.fori_loop(0, TILES, gather, 0)


def columns_call(place, offsets, bands, otf, tab):
    return pl.pallas_call(
        columns_kernel,
        name="column_sums",
        out_shape=(
            jax.ShapeDtypeStruct((DEPTH, 2, SLAB, N), BF16),
            jax.ShapeDtypeStruct((CUTS, SLAB, LANES), F32),
        ),
        grid_spec=pltpu.PrefetchScalarGridSpec(
            num_scalar_prefetch=2,
            grid=(1,),
            in_specs=[
                pl.BlockSpec((GROUP, PLANES, SLAB, LANES), lambda g, p, o: (0, 0, 0, 0)),
                pl.BlockSpec((ROW, TILES, SLAB, LANES), lambda g, p, o: (0, 0, 0, 0)),
                pl.BlockSpec((GROUP, DEPTH, 2, 16, 256), lambda g, p, o: (0, 0, 0, 0, p[0])),
                pl.BlockSpec((GROUP, DEPTH, 2, 16, 256), lambda g, p, o: (0, 0, 0, 0, p[0] + 4)),
            ],
            out_specs=(
                pl.BlockSpec((DEPTH, 2, SLAB, N), lambda g, p, o: (0, 0, 0, 0)),
                pl.BlockSpec((CUTS, SLAB, LANES), lambda g, p, o: (0, 0, 0)),
            ),
            scratch_shapes=[
                pltpu.VMEM((FIELDS, N + PAD, LANES), F32),
                pltpu.VMEM((PLANES, N + PAD, LANES), F32),
                pltpu.VMEM((LANES, LANES), F32),
            ],
        ),
    )(place, offsets, bands, otf, tab, tab)


def finish_kernel(
    numer, power, tab, recon,
    numer_rx, power_rx, den_tx, den_rx, inv_tab, fin_tab, ratio_lo, ratio_hi, half_tx, half_rx,
    lhs, tab_sem, numer_send, numer_recv, power_send, power_recv, den_send, den_recv,
    half_send, half_recv,
):
    r = lax.axis_index("row")
    k = lax.axis_index("cuts")
    z, i = r // GROUP, r % GROUP

    loads = [pltpu.make_async_copy(tab, inv_tab, tab_sem.at[0])]
    for d in range(DEPTH):
        for part in range(2):
            loads.append(
                pltpu.make_async_copy(
                    tab.at[:, d, :, :, pl.ds(part * N, N)],
                    fin_tab.at[d, :, part],
                    tab_sem.at[1 + 2 * d + part],
                )
            )
    for load in loads:
        load.start()

    barrier = pltpu.get_barrier_semaphore()

    def greet_row(o, carry):
        pl.semaphore_signal(
            barrier, inc=1, device_id={"row": lax.rem(r + o, ROW)}, device_id_type=MESH
        )
        return carry

    def greet_cut(o, carry):
        pl.semaphore_signal(
            barrier, inc=1, device_id={"cuts": lax.rem(k + o, CUTS)}, device_id_type=MESH
        )
        return carry

    lax.fori_loop(1, ROW, greet_row, 0)
    lax.fori_loop(1, CUTS, greet_cut, 0)
    pl.semaphore_wait(barrier, ROW - 1 + CUTS - 1)

    def remote(src, dst, send, recv, to):
        return pltpu.make_async_remote_copy(
            src_ref=src, dst_ref=dst, send_sem=send, recv_sem=recv,
            device_id=to, device_id_type=MESH,
        )

    power_copies = []
    for o in range(1, CUTS):
        to = lax.rem(k + o, CUTS)
        copy = remote(power.at[to], power_rx.at[o], power_send.at[o], power_recv.at[o], {"cuts": to})
        copy.start()
        power_copies.append(copy)
    numer_copies = []
    for o in range(1, DEPTH):
        to = lax.rem(z + o, DEPTH)
        copy = remote(
            numer.at[to], numer_rx.at[o], numer_send.at[o], numer_recv.at[o],
            {"row": to * GROUP + i},
        )
        copy.start()
        numer_copies.append(copy)

    ratio_lo[...] = jnp.zeros_like(ratio_lo)
    ratio_hi[...] = jnp.zeros_like(ratio_hi)

    total = power[k]
    for o in range(1, CUTS):
        power_copies[o - 1].wait()
        total = total + power_rx[o]
    den = WIENER + total / float(CUTS * ANGLES)
    den_tx[...] = den
    den_copies = []
    for o in range(1, CUTS):
        to = lax.rem(k + o, CUTS)
        copy = remote(den_tx, den_rx.at[k], den_send.at[o], den_recv.at[o], {"cuts": to})
        copy.start()
        den_copies.append(copy)
    for copy in den_copies:
        copy.wait()
    den_rx[k] = den
    for copy in numer_copies:
        copy.wait()
    for n in range(TILES):
        cols = slice(n * LANES, (n + 1) * LANES)
        over = slice(N + n * LANES, N + (n + 1) * LANES)
        below = den_rx[n]
        re = numer[z, 0, :, cols].astype(F32)
        im = numer[z, 1, :, cols].astype(F32)
        for o in range(1, DEPTH):
            re = re + numer_rx[o, 0, :, cols].astype(F32)
            im = im + numer_rx[o, 1, :, cols].astype(F32)
        re = re / below
        im = im / below
        plus, minus, back = re.astype(BF16), (-im).astype(BF16), (-re).astype(BF16)
        for ref, row in ((ratio_lo, 0), (ratio_hi, 64)):
            ref[row : row + 32, cols] = plus
            ref[row : row + 32, over] = minus
            ref[row + 32 : row + 64, cols] = minus
            ref[row + 32 : row + 64, over] = back

    loads[0].wait()
    contract = (((1,), (1,)), ((), ()))
    half = lax.dot_general(
        inv_tab[:, :, 0].reshape(N // 2, 2 * N), ratio_lo[...], contract,
        preferred_element_type=F32,
    ) + lax.dot_general(
        inv_tab[:, :, 1].reshape(N // 2, 2 * N), ratio_hi[...], contract,
        preferred_element_type=F32,
    )
    half_tx[...] = half.astype(BF16).reshape(ROW, 16, LANES)

    def send_half(o, carry):
        to = lax.rem(r + o, ROW)
        remote(
            half_tx.at[to], half_rx.at[r], half_send.at[o], half_recv.at[o], {"row": to}
        ).start()
        return carry

    lax.fori_loop(1, ROW, send_half, 0)
    for load in loads[1:]:
        load.wait()

    def wait_half(o, carry):
        to = lax.rem(r + o, ROW)
        remote(
            half_tx.at[to], half_rx.at[r], half_send.at[o], half_recv.at[o], {"row": to}
        ).wait()
        return carry

    lax.fori_loop(1, ROW, wait_half, 0)
    half_rx[r] = half_tx[r]

    first = lane_index(16) < 64
    for t in range(ROW // 2):
        even = half_rx[2 * t].astype(F32)
        odd = half_rx[2 * t + 1].astype(F32)
        cols = slice(t * LANES, (t + 1) * LANES)
        lhs[0:16, cols] = jnp.where(first, even, pltpu.roll(odd, 64, 1)).astype(BF16)
        lhs[16:32, cols] = jnp.where(first, pltpu.roll(even, 64, 1), odd).astype(BF16)
    for n in range(4):
        cols = slice(n * 256, (n + 1) * 256)
        recon[:, cols] = jnp.dot(
            lhs[...], fin_tab[:, :, :, :, :, cols].reshape(2 * N, 256), preferred_element_type=F32
        )


def finish_call(numer, power, tab):
    vmem = pl.BlockSpec(memory_space=pltpu.VMEM)
    dma = pltpu.SemaphoreType.DMA
    return pl.pallas_call(
        finish_kernel,
        name="finish",
        out_shape=jax.ShapeDtypeStruct((SLAB, N), F32),
        in_specs=[vmem, vmem, pl.BlockSpec(memory_space=pl.ANY)],
        out_specs=vmem,
        scratch_shapes=[
            pltpu.VMEM((DEPTH, 2, SLAB, N), BF16),
            pltpu.VMEM((CUTS, SLAB, LANES), F32),
            pltpu.VMEM((SLAB, LANES), F32),
            pltpu.VMEM((CUTS, SLAB, LANES), F32),
            pltpu.VMEM((GROUP, DEPTH, 2, 16, 2 * N), BF16),
            pltpu.VMEM((DEPTH, GROUP, 2, 2, 16, N), BF16),
            pltpu.VMEM((LANES, 2 * N), BF16),
            pltpu.VMEM((LANES, 2 * N), BF16),
            pltpu.VMEM((ROW, 16, LANES), BF16),
            pltpu.VMEM((ROW, 16, LANES), BF16),
            pltpu.VMEM((SLAB, 2 * N), BF16),
            dma((1 + 2 * DEPTH,)),
            dma((DEPTH,)), dma((DEPTH,)),
            dma((CUTS,)), dma((CUTS,)), dma((CUTS,)), dma((CUTS,)),
            dma((ROW,)), dma((ROW,)),
        ],
        compiler_params=pltpu.CompilerParams(collective_id=1, has_side_effects=True),
    )(numer, power, tab)


def solution(mesh):
    tab_host = table()

    def shards(raw, otf, offsets, phase_order, unmix):
        tab = jnp.asarray(tab_host)
        r = lax.axis_index("row")
        place = jnp.stack([r // GROUP, r % GROUP]).astype(jnp.int32)
        offsets = offsets.reshape(-1)
        bands, otf_own = rows_call(
            offsets, phase_order.reshape(-1), unmix.reshape(-1),
            raw.reshape(ANGLES * PHASES * SLAB, N), tab, otf[0],
        )
        bands, otf_all = exchange_call(bands, otf_own)
        otf_all = otf_all.reshape(ROW, TILES, SLAB, LANES)
        numer, power = columns_call(place, offsets, bands, otf_all, tab)
        return finish_call(numer, power, tab)[None]

    in_specs = (P("cuts", None, None, "row", None), P("cuts", "row", None), P(), P(), P())
    return jax.shard_map(
        shards, mesh=mesh, in_specs=in_specs, out_specs=P("cuts", "row", None), check_vma=False
    )
```
